256 devices in a mesh: layer: 4 (over y_hi, core), latent: 64 (over x, z, y_lo).
Axes of the slice: x: 4, y: 4 (y_hi: 2, y_lo: 2; y = y_hi * 2 + y_lo), z: 8, core: 2. Of those that a mesh axis runs over, the one named last changes fastest.
Arguments:
- inputs: bfloat16 [4, 128, 4096], P('layer', 'latent'), may hold values from -6 to 6
- targets: bfloat16 [4, 128, 4096], P('layer', 'latent'), may hold values from -6 to 6
- w_enc: bfloat16 [4, 4096, 8192], P('layer', None, 'latent'), may hold values from -0.09375 to 0.09375
- b_enc: float32 [4, 8192], P('layer', 'latent'), may hold values from -3 to 3
- w_dec: bfloat16 [4, 4, 8192, 4096], P('layer', None, 'latent'), may hold values from -0.03125 to 0.03125
- b_dec: float32 [4, 4096], P('layer'), may hold values from -3 to 3
Outputs:
- grad_enc: bfloat16 [4, 4096, 8192], P('layer', None, 'latent')
- grad_benc: float32 [4, 8192], P('layer', 'latent')
- grad_dec: bfloat16 [4, 4, 8192, 4096], P('layer', None, 'latent')
- grad_bdec: float32 [4, 4096], P('layer')
The draws below stay inside these ranges and needn't reach their ends.
All inputs are finite; a program needn't handle non-finite values.
Results may differ from the reference program's by a relative error of at most 0.0057.
Values may be sent and summed in bfloat16 or wider, within the bound.
No kernel may reach another device: no remote copies, remote signals or barrier semaphores. Data moves between devices by JAX's collectives and lax.ppermute only.
A program may use at most 64 MiB of HBM per device.

```python
import jax
import jax.numpy as jnp
from jax import lax

D = 4096
LATENTS = 8192
TOKENS = 128
LAYERS = 4


def levels(rng, dims, cuts, least, high):
    factor_of = 1.0
    for axis_at, blocks in cuts:
        draws = jax.random.uniform(jax.random.fold_in(jax.random.fold_in(rng, 6), axis_at), (blocks,), jnp.float32, least / len(cuts), high / len(cuts))
        factor_of = factor_of * jnp.repeat(jnp.exp(draws), dims[axis_at] // blocks).reshape((-1,) + (1,) * (len(dims) - 1 - axis_at))
    return factor_of


def scatter_about(own_key, shape, width, most, cuts=(), dtype=jnp.bfloat16):
    result = width * jax.random.normal(own_key, shape, jnp.float32)
    if cuts:
        result = result * levels(own_key, shape, cuts, -0.22, 0.18)
    return jnp.clip(result, -most, most).astype(dtype)


def setup_inputs(seed: int = 0) -> dict:
    seeds = jax.random.split(jax.random.key(seed), 7)
    inputs = scatter_about(seeds[0], (LAYERS, TOKENS, D), 1.0, 6.0, ((0, 4), (1, 64)))
    targets = scatter_about(seeds[1], (LAYERS, TOKENS, D), 1.0, 6.0, ((0, 4), (1, 64)))
    w_enc = scatter_about(seeds[2], (LAYERS, D, LATENTS), D ** -0.5, 0.09375, ((0, 4), (2, 64)))
    b_enc = scatter_about(seeds[3], (LAYERS, LATENTS), 0.5, 3.0, ((0, 4), (1, 64)), jnp.float32)
    w_dec = scatter_about(seeds[4], (LAYERS, LAYERS, LATENTS, D), (LAYERS * LATENTS) ** -0.5, 0.03125, ((0, 4), (2, 64)))
    b_dec = scatter_about(seeds[5], (LAYERS, D), 0.5, 3.0, ((0, 4),), jnp.float32)
    return {"inputs": inputs, "targets": targets, "w_enc": w_enc, "b_enc": b_enc, "w_dec": w_dec, "b_dec": b_dec}


penalty = 0.5
eps = 1e-06

def reference(inputs, targets, w_enc, b_enc, w_dec, b_dec):
    pres = []
    acts = []
    for s in range(LAYERS):
        pre = jnp.dot(inputs[s], w_enc[s], preferred_element_type=jnp.float32) + b_enc[s]
        pres.append(pre)
        positive = jnp.maximum(pre, 0.0)
        acts.append((positive * positive).astype(jnp.bfloat16))
    err_low = []
    bias_rows = []
    for t in range(LAYERS):
        recon = jnp.zeros((TOKENS, D), jnp.float32)
        for s in range(t + 1):
            recon = recon + jnp.dot(acts[s], w_dec[s, t], preferred_element_type=jnp.float32)
        error = recon + b_dec[t] - targets[t].astype(jnp.float32)
        bias_rows.append(lax.optimization_barrier(jnp.sum(error, axis=0)))
        err_low.append(error.astype(jnp.bfloat16))
    grad_enc = []
    grad_benc = []
    grad_dec = []
    for s in range(LAYERS):
        total_sq = jnp.zeros((LATENTS,), jnp.float32)
        back = jnp.zeros((TOKENS, LATENTS), jnp.float32)
        for t in range(s, LAYERS):
            wide = w_dec[s, t].astype(jnp.float32)
            total_sq = total_sq + lax.optimization_barrier(jnp.sum(wide * wide, axis=1))
            back = back + lax.dot_general(err_low[t], w_dec[s, t], (((1,), (1,)), ((), ())), preferred_element_type=jnp.float32)
        norms = jnp.sqrt(total_sq + eps)
        d_act = back + penalty * norms[None, :]
        d_pre = d_act * 2.0 * jnp.maximum(pres[s], 0.0)
        grad_benc.append(lax.optimization_barrier(jnp.sum(d_pre, axis=0)))
        d_low = d_pre.astype(jnp.bfloat16)
        grad_enc.append(lax.dot_general(inputs[s], d_low, (((0,), (0,)), ((), ())), preferred_element_type=jnp.float32).astype(jnp.bfloat16))
        act_total = lax.optimization_barrier(jnp.sum(acts[s].astype(jnp.float32), axis=0))
        scale = penalty * act_total / norms
        rows = []
        for t in range(LAYERS):
            if t < s:
                rows.append(jnp.zeros((LATENTS, D), jnp.bfloat16))
            else:
                mse = lax.dot_general(acts[s], err_low[t], (((0,), (0,)), ((), ())), preferred_element_type=jnp.float32)
                rows.append((mse + scale[:, None] * w_dec[s, t].astype(jnp.float32)).astype(jnp.bfloat16))
        grad_dec.append(jnp.stack(rows))
    return (jnp.stack(grad_enc), jnp.stack(grad_benc), jnp.stack(grad_dec), jnp.stack(bias_rows))
```

```python
import jax
import jax.numpy as jnp
from jax import lax
from jax.experimental import pallas as pl
from jax.experimental.pallas import tpu as pltpu
from jax.sharding import Mesh, PartitionSpec as P

penalty = 0.5
eps = 1e-06
bf16 = jnp.bfloat16
f32 = jnp.float32


def shift(v, axis, by):
    n = lax.axis_size(axis)
    return lax.ppermute(v, axis, [(i, (i + by) % n) for i in range(n)])


def gather_z(v):
    n = lax.axis_size("z")
    return lax.all_to_all(
        jnp.broadcast_to(v, (n, *v.shape)), "z", split_axis=0, concat_axis=0, tiled=True
    )


def gather_x(v):
    n = lax.axis_size("x")
    return [v] + [shift(v, "x", -d) for d in range(1, n)]


def recon_kernel(order, valid, act, w, out, squares):
    i = pl.program_id(0)
    use = valid[i] > 0

    @pl.when(i == 0)
    def _():
        squares[...] = jnp.zeros_like(squares)

    @pl.when(use)
    def _():
        wide = w[0].astype(f32)
        squares[...] += jnp.sum(wide * wide, axis=1, keepdims=True)
        out[0] = jnp.dot(act[...], w[0], preferred_element_type=f32).astype(bf16)

    @pl.when(jnp.logical_not(use))
    def _():
        out[0] = jnp.zeros(out.shape[1:], bf16)


def recon_part(order, valid, act, w):
    n, k = act.shape
    d = w.shape[2]
    slots = order.shape[0]
    return pl.pallas_call(
        recon_kernel,
        grid_spec=pltpu.PrefetchScalarGridSpec(
            num_scalar_prefetch=2,
            grid=(slots,),
            in_specs=[
                pl.BlockSpec((n, k), lambda i, o, v: (0, 0)),
                pl.BlockSpec((1, k, d), lambda i, o, v: (o[i], 0, 0)),
            ],
            out_specs=[
                pl.BlockSpec((1, n, d), lambda i, o, v: (i, 0, 0)),
                pl.BlockSpec((k, 1), lambda i, o, v: (0, 0)),
            ],
        ),
        out_shape=[
            jax.ShapeDtypeStruct((slots, n, d), bf16),
            jax.ShapeDtypeStruct((k, 1), f32),
        ],
        name="recon_part",
    )(order, valid, act, w)


def grad_kernel(order, valid, act, scale, w, e, *refs):
    back, out = refs[-2:]
    i = pl.program_id(0)
    use = valid[i] > 0

    @pl.when(i == 0)
    def _():
        back[...] = jnp.zeros_like(back)

    @pl.when(use)
    def _():
        back[...] += lax.dot_general(
            e[0], w[0], (((1,), (1,)), ((), ())), preferred_element_type=f32
        )
        mse = lax.dot_general(
            act[...], e[0], (((0,), (0,)), ((), ())), preferred_element_type=f32
        )
        out[0] = (mse + scale[...] * w[0].astype(f32)).astype(bf16)

    @pl.when(jnp.logical_not(use))
    def _():
        out[0] = jnp.zeros(out.shape[1:], bf16)


def grad_part(order, valid, act, scale, w, e, prior):
    n, k = act.shape
    d = w.shape[2]
    slots = order.shape[0]
    extra = [] if prior is None else [prior]
    return pl.pallas_call(
        grad_kernel,
        grid_spec=pltpu.PrefetchScalarGridSpec(
            num_scalar_prefetch=2,
            grid=(slots,),
            in_specs=[
                pl.BlockSpec((n, k), lambda i, o, v: (0, 0)),
                pl.BlockSpec((k, 1), lambda i, o, v: (0, 0)),
                pl.BlockSpec((1, k, d), lambda i, o, v: (o[i], 0, 0)),
                pl.BlockSpec((1, n, d), lambda i, o, v: (i, 0, 0)),
            ]
            + [pl.BlockSpec(memory_space=pl.ANY) for _ in extra],
            out_specs=[
                pl.BlockSpec((n, k), lambda i, o, v: (0, 0)),
                pl.BlockSpec((1, k, d), lambda i, o, v: (o[i], 0, 0)),
            ],
        ),
        out_shape=[
            jax.ShapeDtypeStruct((n, k), f32),
            jax.ShapeDtypeStruct(w.shape, bf16),
        ],
        input_output_aliases={} if prior is None else {6: 1},
        name="grad_part",
    )(order, valid, act, scale, w, e, *extra)


def enc_kernel(whole, d_low, out):
    out[...] = lax.dot_general(
        whole[...], d_low[...], (((0,), (0,)), ((), ())), preferred_element_type=f32
    ).astype(bf16)


def enc_part(whole, d_low):
    n, d = whole.shape
    k = d_low.shape[1]
    steps = 4
    return pl.pallas_call(
        enc_kernel,
        grid=(steps,),
        in_specs=[
            pl.BlockSpec((n, d // steps), lambda i: (0, i)),
            pl.BlockSpec((n, k), lambda i: (0, 0)),
        ],
        out_specs=pl.BlockSpec((d // steps, k), lambda i: (i, 0)),
        out_shape=jax.ShapeDtypeStruct((d, k), bf16),
        name="enc_part",
    )(whole, d_low)


def local(inputs, targets, w_enc, b_enc, w_dec, b_dec):
    high = lax.axis_index("y_hi")
    core = lax.axis_index("core")
    source = high * 2 + core
    decoders = w_dec[0]
    width = decoders.shape[2]
    mine = jnp.stack([core, core + 2]).astype(jnp.int32)
    theirs = jnp.stack([1 - core, 3 - core]).astype(jnp.int32)
    mine_valid = (mine >= source).astype(jnp.int32)
    theirs_valid = (theirs >= source).astype(jnp.int32)

    with jax.named_scope("gather_in"):
        rows = gather_z(inputs[0]).reshape(-1, width)
        rows = jnp.concatenate([rows, shift(rows, "y_lo", 1)], axis=0)
        whole = jnp.concatenate(gather_x(rows), axis=0)
    pre = jnp.dot(whole, w_enc[0], preferred_element_type=f32) + b_enc[0]
    positive = jnp.maximum(pre, 0.0)
    act = (positive * positive).astype(bf16)

    give, squares_theirs = recon_part(theirs, theirs_valid, act, decoders)
    got = shift(give, "core", 1)
    keep, squares_mine = recon_part(mine, mine_valid, act, decoders)
    part = (keep.astype(f32) + got.astype(f32)).astype(bf16)

    n_x = lax.axis_size("x")
    with jax.named_scope("reduce_x"):
        part = part.reshape(2, n_x, -1, width)
        total = part[:, 0].astype(f32)
        for d in range(1, n_x):
            total = total + shift(part[:, d], "x", d).astype(f32)
        part = total.astype(bf16)
    with jax.named_scope("reduce_y"):
        part = part.reshape(2, 2, -1, width)
        part = part[:, 0].astype(f32) + shift(part[:, 1], "y_lo", 1).astype(f32)
        part = part.astype(bf16)
    with jax.named_scope("reduce_z"):
        n_z = lax.axis_size("z")
        part = jnp.moveaxis(part.reshape(2, n_z, -1, width), 1, 0)
        part = lax.all_to_all(part, "z", split_axis=0, concat_axis=0, tiled=True)
        recon = jnp.sum(part.astype(f32), axis=0)
    offset = b_dec[0] - targets[0].astype(f32)
    with jax.named_scope("reduce_hi"):
        first = recon[0] + offset
        second = recon[1] + jnp.where(high == 1, offset, 0.0)
        second = second + shift(second, "y_hi", 1)
    low = jnp.stack([first, second]).astype(bf16)

    with jax.named_scope("gather_err"):
        low = jnp.moveaxis(gather_z(low), 0, 1).reshape(2, -1, width)
        low = jnp.concatenate([low, shift(low, "y_lo", 1)], axis=1)
        errors = jnp.concatenate(gather_x(low), axis=1)
    other = shift(errors, "core", 1)
    own = jnp.where(high == 0, errors[0], errors[1])
    grad_bdec = jnp.sum(own.astype(f32), axis=0)[None, :]

    norms = jnp.sqrt(squares_mine + squares_theirs + eps)
    act_total = jnp.sum(act.astype(f32), axis=0)
    scale = penalty * act_total[:, None] / norms
    back_mine, grad_dec = grad_part(mine, mine_valid, act, scale, decoders, errors, None)
    back_theirs, grad_dec = grad_part(
        theirs, theirs_valid, act, scale, decoders, other, grad_dec
    )
    d_act = back_mine + back_theirs + penalty * norms.reshape(1, -1)
    d_pre = d_act * 2.0 * positive
    grad_benc = jnp.sum(d_pre, axis=0)[None, :]
    grad_enc = enc_part(whole, d_pre.astype(bf16))[None]
    return (grad_enc, grad_benc, grad_dec[None], grad_bdec)


def solution(mesh):
    parts = Mesh(
        mesh.devices.reshape(2, 2, 4, 8, 2), ("y_hi", "core", "x", "z", "y_lo")
    )
    layer = ("y_hi", "core")
    latent = ("x", "z", "y_lo")
    placed = (
        P(layer, latent, None),
        P(layer, latent, None),
        P(layer, None, latent),
        P(layer, latent),
        P(layer, None, latent, None),
        P(layer, None),
    )
    return jax.shard_map(
        local,
        mesh=parts,
        in_specs=placed,
        out_specs=(
            P(layer, None, latent),
            P(layer, latent),
            P(layer, None, latent, None),
            P(layer, None),
        ),
        check_vma=False,
    )
```

```python
import jax
import jax.numpy as jnp
from jax import lax
from jax.experimental import pallas as pl
from jax.experimental.pallas import tpu as pltpu
from jax.sharding import Mesh, PartitionSpec as P

penalty = 0.5
eps = 1e-06
bf16 = jnp.bfloat16
f32 = jnp.float32
grant = 16 << 20


def shift(v, axis, by):
    n = lax.axis_size(axis)
    return lax.ppermute(v, axis, [(i, (i + by) % n) for i in range(n)])


def gather_z(v):
    n = lax.axis_size("z")
    return lax.all_to_all(
        jnp.broadcast_to(v, (n, *v.shape)), "z", split_axis=0, concat_axis=0, tiled=True
    )


def gather_x(v):
    n = lax.axis_size("x")
    return [v] + [shift(v, "x", -d) for d in range(1, n)]


def spec(shape, index):
    return pl.BlockSpec(shape, index)


def hold_kernel(when, w, out):
    pltpu.sync_copy(w, out)


def hold_part(when, w):
    return pl.pallas_call(
        hold_kernel,
        grid_spec=pltpu.PrefetchScalarGridSpec(
            num_scalar_prefetch=1,
            grid=(1,),
            in_specs=[pl.BlockSpec(memory_space=pl.ANY)],
            out_specs=pl.BlockSpec(memory_space=pltpu.VMEM),
        ),
        out_shape=jax.ShapeDtypeStruct(w.shape, w.dtype),
        cost_estimate=pl.CostEstimate(
            flops=w.size * 128, bytes_accessed=2 * w.size, transcendentals=0
        ),
        compiler_params=pltpu.CompilerParams(vmem_limit_bytes=grant),
        name="hold_part",
    )(when, w)


def product(valid, act, w):
    got = jnp.dot(act[...], w[0], preferred_element_type=f32)
    return jnp.where(valid[0] > 0, got, 0.0)


def give_kernel(order, valid, act, w, out):
    out[...] = product(valid, act, w).astype(bf16)


def keep_kernel(order, valid, act, w, got, *outs):
    total = (product(valid, act, w) + got[...].astype(f32)).astype(bf16)
    rows = outs[0].shape[0]
    for i, out in enumerate(outs):
        out[...] = total[i * rows : (i + 1) * rows]


def recon_part(target, valid, act, w, got=None, pieces=1):
    n, k = act.shape
    d = w.shape[2]
    wide = d
    rows = n // pieces
    ins = [
        spec((n, k), lambda j, o, v: (0, 0)),
        spec((1, k, wide), lambda j, o, v: (o[0], 0, j)),
    ]
    args = [target[None], valid[None], act, w]
    if got is not None:
        ins.append(spec((n, wide), lambda j, o, v: (0, j)))
        args.append(got)
    return pl.pallas_call(
        give_kernel if got is None else keep_kernel,
        grid_spec=pltpu.PrefetchScalarGridSpec(
            num_scalar_prefetch=2,
            grid=(1,),
            in_specs=ins,
            out_specs=[spec((rows, wide), lambda j, o, v: (0, j)) for _ in range(pieces)],
        ),
        out_shape=[jax.ShapeDtypeStruct((rows, d), bf16) for _ in range(pieces)],
        cost_estimate=pl.CostEstimate(
            flops=2 * n * k * d, bytes_accessed=2 * (n + k) * d, transcendentals=0
        ),
        compiler_params=pltpu.CompilerParams(vmem_limit_bytes=grant),
        name="recon_part",
    )(*args)


def side_kernel(valid, w, whole, act, turned, scale, charge, squares):
    j = pl.program_id(0)

    @pl.when(j == 0)
    def _():
        squares[...] = jnp.zeros_like(squares)

    for t in range(w.shape[0]):

        @pl.when(valid[t] > 0)
        def _():
            wide = w[t].astype(f32)
            squares[...] += jnp.sum(wide * wide, axis=1, keepdims=True)

    turned[...] = whole[...].T

    @pl.when(j == pl.num_programs(0) - 1)
    def _():
        norms = jnp.sqrt(squares[...] + eps)
        total = jnp.sum(act[...].astype(f32).T, axis=1, keepdims=True)
        scale[...] = penalty * total / norms
        charge[...] = (penalty * jnp.broadcast_to(norms, act.shape).T)[:1]


def side_part(valid, w, whole, act):
    n, k = act.shape
    t, _, d = w.shape
    wide = d // 4
    return pl.pallas_call(
        side_kernel,
        grid_spec=pltpu.PrefetchScalarGridSpec(
            num_scalar_prefetch=1,
            grid=(4,),
            in_specs=[
                spec((t, k, wide), lambda j, v: (0, 0, j)),
                spec((n, wide), lambda j, v: (0, j)),
                spec((n, k), lambda j, v: (0, 0)),
            ],
            out_specs=[
                spec((wide, n), lambda j, v: (j, 0)),
                spec((k, 1), lambda j, v: (0, 0)),
                spec((1, k), lambda j, v: (0, 0)),
            ],
            scratch_shapes=[pltpu.VMEM((k, 1), f32)],
        ),
        out_shape=[
            jax.ShapeDtypeStruct((d, n), bf16),
            jax.ShapeDtypeStruct((k, 1), f32),
            jax.ShapeDtypeStruct((1, k), f32),
        ],
        cost_estimate=pl.CostEstimate(
            flops=8 * n * k * d, bytes_accessed=2 * (t * k + 2 * n) * d, transcendentals=0
        ),
        compiler_params=pltpu.CompilerParams(vmem_limit_bytes=grant),
        name="side_part",
    )(valid, w, whole, act)


def grad_kernel(order, valid, own, act, scale, w, e0, e1, *refs):
    back, out, bias = refs[-3:]
    i = pl.program_id(0)
    j = pl.program_id(1)
    use = valid[i] > 0

    @pl.when(j == 0)
    def _():
        back[...] = jnp.zeros_like(back)

    for slot, e in enumerate((e0, e1)):

        @pl.when(use & (i == slot))
        def _():
            back[0] += lax.dot_general(
                e[...], w[0], (((1,), (1,)), ((), ())), preferred_element_type=f32
            )
            mse = lax.dot_general(
                act[0], e[...], (((0,), (0,)), ((), ())), preferred_element_type=f32
            )
            out[0] = (mse + scale[...] * w[0].astype(f32)).astype(bf16)

        @pl.when((own[0] == order[i]) & (i == slot))
        def _():
            bias[0] = jnp.sum(e[...].astype(f32), axis=0, keepdims=True)

    @pl.when(jnp.logical_not(use))
    def _():
        out[0] = jnp.zeros(out.shape[1:], bf16)

    @pl.when(own[0] != order[i])
    def _():
        bias[0] = jnp.zeros(bias.shape[1:], f32)


def grad_part(order, valid, own, act, scale, w, e0, e1, prior):
    slots, n, k = act.shape
    d = w.shape[2]
    steps = 1
    wide = d // steps
    extra = [] if prior is None else [prior]
    return pl.pallas_call(
        grad_kernel,
        grid_spec=pltpu.PrefetchScalarGridSpec(
            num_scalar_prefetch=3,
            grid=(slots, steps),
            in_specs=[
                spec((1, n, k), lambda i, j, o, v, s: (i, 0, 0)),
                spec((k, 1), lambda i, j, o, v, s: (0, 0)),
                spec((1, k, wide), lambda i, j, o, v, s: (o[i], 0, j)),
                spec((n, wide), lambda i, j, o, v, s: (0, jnp.where(i == 0, j, steps - 1))),
                spec((n, wide), lambda i, j, o, v, s: (0, jnp.where(i == 0, 0, j))),
            ]
            + [pl.BlockSpec(memory_space=pl.ANY) for _ in extra],
            out_specs=[
                spec((1, n, k), lambda i, j, o, v, s: (i, 0, 0)),
                spec((1, k, wide), lambda i, j, o, v, s: (o[i], 0, j)),
                spec((1, 1, wide), lambda i, j, o, v, s: (i, 0, j)),
            ],
        ),
        out_shape=[
            jax.ShapeDtypeStruct((slots, n, k), f32),
            jax.ShapeDtypeStruct(w.shape, bf16),
            jax.ShapeDtypeStruct((slots, 1, d), f32),
        ],
        input_output_aliases={} if prior is None else {8: 1},
        cost_estimate=pl.CostEstimate(
            flops=8 * n * k * d, bytes_accessed=12 * n * d, transcendentals=0
        ),
        compiler_params=pltpu.CompilerParams(vmem_limit_bytes=grant),
        name="grad_part",
    )(order, valid, own, act, scale, w, e0, e1, *extra)


def enc_kernel(turned, mine, theirs, charge, positive, out, bias, d_low):
    @pl.when(pl.program_id(0) == 0)
    def _():
        swapped = mine[1] + theirs[1]
        n = swapped.shape[0]
        rows = n // 8
        order = [swapped[(y * 4 + x) * rows :][:rows] for x in range(4) for y in range(2)]
        d_act = mine[0] + theirs[0] + jnp.concatenate(order, axis=0) + charge[...]
        d_pre = d_act * 2.0 * positive[...]
        bias[...] = jnp.sum(d_pre, axis=0, keepdims=True)
        d_low[...] = d_pre.astype(bf16)

    out[...] = jnp.dot(turned[...], d_low[...], preferred_element_type=f32).astype(bf16)


def enc_part(turned, mine, theirs, charge, positive):
    d, n = turned.shape
    k = charge.shape[1]
    steps = 4
    return pl.pallas_call(
        enc_kernel,
        grid=(steps,),
        in_specs=[
            spec((d // steps, n), lambda j: (j, 0)),
            spec((2, n, k), lambda j: (0, 0, 0)),
            spec((2, n, k), lambda j: (0, 0, 0)),
            spec((1, k), lambda j: (0, 0)),
            spec((n, k), lambda j: (0, 0)),
        ],
        out_specs=[
            spec((d // steps, k), lambda j: (j, 0)),
            spec((1, k), lambda j: (0, 0)),
        ],
        out_shape=[
            jax.ShapeDtypeStruct((d, k), bf16),
            jax.ShapeDtypeStruct((1, k), f32),
        ],
        scratch_shapes=[pltpu.VMEM((n, k), bf16)],
        compiler_params=pltpu.CompilerParams(vmem_limit_bytes=grant),
        name="enc_part",
    )(turned, mine, theirs, charge, positive)


def after(v, *earlier):
    return lax.optimization_barrier((v, *earlier))[0]


def added(first, rest):
    total = first.astype(f32)
    for v in rest:
        total = total + v.astype(f32)
    return total.astype(bf16)


def local(inputs, targets, w_enc, b_enc, w_dec, b_dec):
    high = lax.axis_index("y_hi")
    core = lax.axis_index("core")
    source = high * 2 + core
    decoders = w_dec[0]
    depth, k, width = decoders.shape
    n_x = lax.axis_size("x")
    n_z = lax.axis_size("z")
    mine = jnp.stack([core, core + 2]).astype(jnp.int32)
    theirs = jnp.stack([1 - core, 3 - core]).astype(jnp.int32)
    mine_valid = (mine >= source).astype(jnp.int32)
    theirs_valid = (theirs >= source).astype(jnp.int32)

    with jax.named_scope("gather_in"):
        rows = gather_z(inputs[0]).reshape(-1, width)
        rows = jnp.concatenate([rows, shift(rows, "y_lo", 1)], axis=0)
        decoders = hold_part(after(mine, rows), decoders)
        whole = jnp.concatenate(gather_x(rows), axis=0)
    pre = jnp.dot(whole, w_enc[0], preferred_element_type=f32) + b_enc[0]
    positive = jnp.maximum(pre, 0.0)
    act = (positive * positive).astype(bf16)
    turned_act = jnp.moveaxis(act.reshape(n_x, 2, -1, k), 1, 0).reshape(-1, k)
    acts = jnp.stack([act, turned_act])

    (give1,) = recon_part(theirs[1], theirs_valid[1], turned_act, decoders)
    got1 = shift(give1, "core", 1)
    (give0,) = recon_part(theirs[0], theirs_valid[0], after(act, give1), decoders)
    got0 = shift(give0, "core", 1)
    part1 = recon_part(
        mine[1], mine_valid[1], after(turned_act, give0), decoders, got1, 2
    )
    part0 = recon_part(
        mine[0], mine_valid[0], after(act, part1[0]), decoders, got0, n_x
    )

    all_valid = (jnp.arange(depth, dtype=jnp.int32) >= source).astype(jnp.int32)
    turned, scale, charge = side_part(after(all_valid, part0[0]), decoders, whole, act)

    with jax.named_scope("reduce_one"):
        come0 = [shift(part0[d], "x", d) for d in range(1, n_x)]
        come1 = shift(part1[1], "y_lo", 1)
        sum0 = added(part0[0], come0)
        sum1 = added(part1[0], [come1])
        sum1 = after(sum1, scale)
    with jax.named_scope("reduce_two"):
        half = sum0.shape[0] // 2
        piece = sum1.shape[0] // n_x
        come0 = shift(sum0[half:], "y_lo", 1)
        come1 = [
            shift(sum1[d * piece : (d + 1) * piece], "x", d) for d in range(1, n_x)
        ]
        part = jnp.stack([added(sum0[:half], [come0]), added(sum1[:piece], come1)])
    with jax.named_scope("reduce_z"):
        part = jnp.moveaxis(part.reshape(2, n_z, -1, width), 1, 0)
        part = lax.all_to_all(part, "z", split_axis=0, concat_axis=0, tiled=True)
        recon = jnp.sum(part.astype(f32), axis=0)
    offset = b_dec[0] - targets[0].astype(f32)
    with jax.named_scope("reduce_hi"):
        first = recon[0] + offset
        second = recon[1] + jnp.where(high == 1, offset, 0.0)
        second = second + shift(second, "y_hi", 1)
    low = jnp.stack([first, second]).astype(bf16)

    with jax.named_scope("gather_err"):
        low = jnp.moveaxis(gather_z(low), 0, 1).reshape(2, -1, width)
        rows0 = jnp.concatenate([low[0], shift(low[0], "y_lo", 1)], axis=0)
        rows1 = jnp.concatenate(gather_x(low[1]), axis=0)
        errors0 = jnp.concatenate(gather_x(rows0), axis=0)
        errors1 = jnp.concatenate([rows1, shift(rows1, "y_lo", 1)], axis=0)
        other0 = shift(errors0, "core", 1)
        other1 = shift(errors1, "core", 1)

    own = source.astype(jnp.int32)[None]
    back, grad_dec, bias = grad_part(
        mine, mine_valid, own, acts, scale, decoders, errors0, errors1, None
    )
    grad_bdec = bias[0] + bias[1]
    others, grad_dec, _ = grad_part(
        theirs, theirs_valid, own, acts, scale, decoders, other0, other1, grad_dec
    )
    grad_enc, grad_benc = enc_part(turned, back, others, charge, positive)
    return (grad_enc[None], grad_benc, grad_dec[None], grad_bdec)


def solution(mesh):
    parts = Mesh(
        mesh.devices.reshape(2, 2, 4, 8, 2), ("y_hi", "core", "x", "z", "y_lo")
    )
    layer = ("y_hi", "core")
    latent = ("x", "z", "y_lo")
    placed = (
        P(layer, latent, None),
        P(layer, latent, None),
        P(layer, None, latent),
        P(layer, latent),
        P(layer, None, latent, None),
        P(layer, None),
    )
    return jax.shard_map(
        local,
        mesh=parts,
        in_specs=placed,
        out_specs=(
            P(layer, None, latent),
            P(layer, latent),
            P(layer, None, latent, None),
            P(layer, None),
        ),
        check_vma=False,
    )
```

```python
import jax
import jax.numpy as jnp
from jax import lax
from jax.experimental import pallas as pl
from jax.experimental.pallas import tpu as pltpu
from jax.sharding import Mesh, PartitionSpec as P

penalty = 0.5
eps = 1e-06
bf16 = jnp.bfloat16
f32 = jnp.float32
grant = 16 << 20


def length(axis):
    names = axis if isinstance(axis, tuple) else (axis,)
    n = 1
    for name in names:
        n *= lax.axis_size(name)
    return n


def shift(v, axis, by):
    n = length(axis)
    return lax.ppermute(v, axis, [(i, (i + by) % n) for i in range(n)])


def gather_z(v):
    n = lax.axis_size("z")
    return lax.all_to_all(
        jnp.broadcast_to(v, (n, *v.shape)), "z", split_axis=0, concat_axis=0, tiled=True
    )


def gather_ring(v, axis):
    return [v] + [shift(v, axis, -d) for d in range(1, length(axis))]


def spec(shape, index):
    return pl.BlockSpec(shape, index)


def hold_kernel(when, w, out):
    pltpu.sync_copy(w, out)


def hold_part(when, w):
    return pl.pallas_call(
        hold_kernel,
        grid_spec=pltpu.PrefetchScalarGridSpec(
            num_scalar_prefetch=1,
            grid=(1,),
            in_specs=[pl.BlockSpec(memory_space=pl.ANY)],
            out_specs=pl.BlockSpec(memory_space=pltpu.VMEM),
        ),
        out_shape=jax.ShapeDtypeStruct(w.shape, w.dtype),
        cost_estimate=pl.CostEstimate(
            flops=w.size * 128, bytes_accessed=2 * w.size, transcendentals=0
        ),
        compiler_params=pltpu.CompilerParams(vmem_limit_bytes=grant),
        name="hold_part",
    )(when, w)


def product(valid, act, w):
    got = jnp.dot(act[...], w[0], preferred_element_type=f32)
    return jnp.where(valid[0] > 0, got, 0.0)


def give_kernel(order, valid, act, w, out):
    out[...] = product(valid, act, w).astype(bf16)


def keep_kernel(order, valid, act, w, got, *outs):
    total = (product(valid, act, w) + got[...].astype(f32)).astype(bf16)
    rows = outs[0].shape[0]
    for i, out in enumerate(outs):
        out[...] = total[i * rows : (i + 1) * rows]


def recon_part(target, valid, act, w, got=None, pieces=1):
    n, k = act.shape
    d = w.shape[2]
    wide = d
    rows = n // pieces
    ins = [
        spec((n, k), lambda j, o, v: (0, 0)),
        spec((1, k, wide), lambda j, o, v: (o[0], 0, j)),
    ]
    args = [target[None], valid[None], act, w]
    if got is not None:
        ins.append(spec((n, wide), lambda j, o, v: (0, j)))
        args.append(got)
    return pl.pallas_call(
        give_kernel if got is None else keep_kernel,
        grid_spec=pltpu.PrefetchScalarGridSpec(
            num_scalar_prefetch=2,
            grid=(1,),
            in_specs=ins,
            out_specs=[spec((rows, wide), lambda j, o, v: (0, j)) for _ in range(pieces)],
        ),
        out_shape=[jax.ShapeDtypeStruct((rows, d), bf16) for _ in range(pieces)],
        cost_estimate=pl.CostEstimate(
            flops=2 * n * k * d, bytes_accessed=2 * (n + k) * d, transcendentals=0
        ),
        compiler_params=pltpu.CompilerParams(vmem_limit_bytes=grant),
        name="recon_part",
    )(*args)


def side_kernel(valid, w, whole, act, turned, scale, charge, squares):
    j = pl.program_id(0)

    @pl.when(j == 0)
    def _():
        squares[...] = jnp.zeros_like(squares)

    for t in range(w.shape[0]):

        @pl.when(valid[t] > 0)
        def _():
            wide = w[t].astype(f32)
            squares[...] += jnp.sum(wide * wide, axis=1, keepdims=True)

    turned[...] = whole[...].T

    @pl.when(j == pl.num_programs(0) - 1)
    def _():
        norms = jnp.sqrt(squares[...] + eps)
        total = jnp.sum(act[...].astype(f32).T, axis=1, keepdims=True)
        scale[...] = penalty * total / norms
        charge[...] = (penalty * jnp.broadcast_to(norms, act.shape).T)[:1]


def side_part(valid, w, whole, act):
    n, k = act.shape
    t, _, d = w.shape
    wide = d // 4
    return pl.pallas_call(
        side_kernel,
        grid_spec=pltpu.PrefetchScalarGridSpec(
            num_scalar_prefetch=1,
            grid=(4,),
            in_specs=[
                spec((t, k, wide), lambda j, v: (0, 0, j)),
                spec((n, wide), lambda j, v: (0, j)),
                spec((n, k), lambda j, v: (0, 0)),
            ],
            out_specs=[
                spec((wide, n), lambda j, v: (j, 0)),
                spec((k, 1), lambda j, v: (0, 0)),
                spec((1, k), lambda j, v: (0, 0)),
            ],
            scratch_shapes=[pltpu.VMEM((k, 1), f32)],
        ),
        out_shape=[
            jax.ShapeDtypeStruct((d, n), bf16),
            jax.ShapeDtypeStruct((k, 1), f32),
            jax.ShapeDtypeStruct((1, k), f32),
        ],
        cost_estimate=pl.CostEstimate(
            flops=8 * n * k * d, bytes_accessed=2 * (t * k + 2 * n) * d, transcendentals=0
        ),
        compiler_params=pltpu.CompilerParams(vmem_limit_bytes=grant),
        name="side_part",
    )(valid, w, whole, act)


def grad_kernel(order, valid, own, act, scale, w, *refs):
    back, out, bias, whole = refs[-4:]
    i = pl.program_id(0)
    use = valid[i] > 0
    rows = refs[0].shape[0]

    for slot in range(2):

        @pl.when(use & (i == slot))
        def _():
            for p in range(4):
                whole[p * rows : (p + 1) * rows] = refs[slot * 4 + p][...]

    @pl.when(use)
    def _():
        e = whole[...]
        back[0] = lax.dot_general(
            e, w[0], (((1,), (1,)), ((), ())), preferred_element_type=f32
        )
        mse = lax.dot_general(
            act[0], e, (((0,), (0,)), ((), ())), preferred_element_type=f32
        )
        out[0] = (mse + scale[...] * w[0].astype(f32)).astype(bf16)

    @pl.when(own[0] == order[i])
    def _():
        bias[0] = jnp.sum(whole[...].astype(f32), axis=0, keepdims=True)

    @pl.when(jnp.logical_not(use))
    def _():
        back[...] = jnp.zeros_like(back)
        out[0] = jnp.zeros(out.shape[1:], bf16)

    @pl.when(own[0] != order[i])
    def _():
        bias[0] = jnp.zeros(bias.shape[1:], f32)


def grad_part(order, valid, own, act, scale, w, e0, e1, prior):
    slots, n, k = act.shape
    d = w.shape[2]
    extra = [] if prior is None else [prior]
    return pl.pallas_call(
        grad_kernel,
        grid_spec=pltpu.PrefetchScalarGridSpec(
            num_scalar_prefetch=3,
            grid=(slots,),
            in_specs=[
                spec((1, n, k), lambda i, o, v, s: (i, 0, 0)),
                spec((k, 1), lambda i, o, v, s: (0, 0)),
                spec((1, k, d), lambda i, o, v, s: (o[i], 0, 0)),
            ]
            + [spec((n // 4, d), lambda i, o, v, s: (0, 0)) for _ in range(8)]
            + [pl.BlockSpec(memory_space=pl.ANY) for _ in extra],
            out_specs=[
                spec((1, n, k), lambda i, o, v, s: (i, 0, 0)),
                spec((1, k, d), lambda i, o, v, s: (o[i], 0, 0)),
                spec((1, 1, d), lambda i, o, v, s: (i, 0, 0)),
            ],
            scratch_shapes=[pltpu.VMEM((n, d), bf16)],
        ),
        out_shape=[
            jax.ShapeDtypeStruct((slots, n, k), f32),
            jax.ShapeDtypeStruct(w.shape, bf16),
            jax.ShapeDtypeStruct((slots, 1, d), f32),
        ],
        input_output_aliases={} if prior is None else {14: 1},
        cost_estimate=pl.CostEstimate(
            flops=8 * n * k * d, bytes_accessed=12 * n * d, transcendentals=0
        ),
        compiler_params=pltpu.CompilerParams(vmem_limit_bytes=24 << 20),
        name="grad_part",
    )(order, valid, own, act, scale, w, *e0, *e1, *extra)


def enc_kernel(turned, mine, theirs, charge, positive, moved, out, bias, d_low):
    @pl.when(pl.program_id(0) == 0)
    def _():
        back = lax.dot_general(
            moved[...],
            mine[1] + theirs[1],
            (((0,), (0,)), ((), ())),
            precision=lax.Precision.HIGHEST,
            preferred_element_type=f32,
        )
        d_act = mine[0] + theirs[0] + back + charge[...]
        d_pre = d_act * 2.0 * positive[...]
        bias[...] = jnp.sum(d_pre, axis=0, keepdims=True)
        d_low[...] = d_pre.astype(bf16)

    out[...] = jnp.dot(turned[...], d_low[...], preferred_element_type=f32).astype(bf16)


def enc_part(turned, mine, theirs, charge, positive, moved):
    d, n = turned.shape
    k = charge.shape[1]
    steps = 4
    return pl.pallas_call(
        enc_kernel,
        grid=(steps,),
        in_specs=[
            spec((d // steps, n), lambda j: (j, 0)),
            spec((2, n, k), lambda j: (0, 0, 0)),
            spec((2, n, k), lambda j: (0, 0, 0)),
            spec((1, k), lambda j: (0, 0)),
            spec((n, k), lambda j: (0, 0)),
            spec((n, n), lambda j: (0, 0)),
        ],
        out_specs=[
            spec((d // steps, k), lambda j: (j, 0)),
            spec((1, k), lambda j: (0, 0)),
        ],
        out_shape=[
            jax.ShapeDtypeStruct((d, k), bf16),
            jax.ShapeDtypeStruct((1, k), f32),
        ],
        scratch_shapes=[pltpu.VMEM((n, k), bf16)],
        compiler_params=pltpu.CompilerParams(vmem_limit_bytes=grant),
        name="enc_part",
    )(turned, mine, theirs, charge, positive, moved)


def after(v, *earlier):
    return lax.optimization_barrier((v, *earlier))[0]


def added(first, rest):
    total = first.astype(f32)
    for v in rest:
        total = total + v.astype(f32)
    return total.astype(bf16)


def local(inputs, targets, w_enc, b_enc, w_dec, b_dec):
    high = lax.axis_index("y_hi")
    core = lax.axis_index("core")
    source = high * 2 + core
    decoders = w_dec[0]
    depth, k, width = decoders.shape
    n_x = lax.axis_size("x")
    n_z = lax.axis_size("z")
    mine = jnp.stack([core, core + 2]).astype(jnp.int32)
    theirs = jnp.stack([1 - core, 3 - core]).astype(jnp.int32)
    mine_valid = (mine >= source).astype(jnp.int32)
    theirs_valid = (theirs >= source).astype(jnp.int32)

    n = 2 * n_x * n_z * 2
    to = lax.broadcasted_iota(jnp.int32, (n, n), 0)
    at = lax.broadcasted_iota(jnp.int32, (n, n), 1)
    ahead = to // (n_x * n_z)
    row = (high * 2 + lax.axis_index("y_lo") + ahead) % 4 // 2
    place = to // n_z % n_x * (4 * n_z) + ahead % 2 * (2 * n_z) + to % n_z * 2 + row
    moved = lax.optimization_barrier((at == place).astype(f32))

    with jax.named_scope("gather_in"):
        rows = gather_z(inputs[0]).reshape(-1, width)
        rows = jnp.concatenate([rows, shift(rows, "y_lo", 1)], axis=0)
        decoders = hold_part(after(mine, rows), decoders)
        whole = jnp.concatenate(gather_ring(rows, "x"), axis=0)
    pre = jnp.dot(whole, w_enc[0], preferred_element_type=f32) + b_enc[0]
    positive = jnp.maximum(pre, 0.0)
    act = (positive * positive).astype(bf16)
    turned_act = jnp.dot(moved.astype(bf16), act, preferred_element_type=f32).astype(bf16)
    acts = jnp.stack([act, turned_act])

    (give1,) = recon_part(theirs[1], theirs_valid[1], turned_act, decoders)
    got1 = shift(give1, "core", 1)
    (give0,) = recon_part(theirs[0], theirs_valid[0], after(act, give1), decoders)
    got0 = shift(give0, "core", 1)
    part1 = recon_part(
        mine[1], mine_valid[1], after(turned_act, give0), decoders, got1, 4
    )
    part0 = recon_part(
        mine[0], mine_valid[0], after(act, part1[0]), decoders, got0, n_x
    )

    ring = ("y_hi", "y_lo")
    with jax.named_scope("reduce_one"):
        come0 = [shift(part0[d], "x", d) for d in range(1, n_x)]
        come1 = [shift(part1[d], ring, d) for d in range(1, 4)]
        all_valid = (jnp.arange(depth, dtype=jnp.int32) >= source).astype(jnp.int32)
        all_valid, come1[0] = lax.optimization_barrier((all_valid, come1[0]))
        turned, scale, charge = side_part(all_valid, decoders, whole, act)
        sum0 = added(part0[0], come0)
        sum1 = added(part1[0], come1)
        sum1 = after(sum1, scale)
    bias, aim = lax.optimization_barrier((b_dec, targets, scale))[:2]
    offset = bias[0] - aim[0].astype(f32)
    with jax.named_scope("offset_hi"):
        offset1 = jnp.where(high == 0, shift(offset[:1], "y_hi", 1), offset[1:])
    with jax.named_scope("reduce_two"):
        half = sum0.shape[0] // 2
        come0 = shift(sum0[half:], "y_lo", 1)
        come1 = [shift(sum1[d * n_z : (d + 1) * n_z], "x", d) for d in range(1, n_x)]
        sum0 = added(sum0[:half], [come0])
        sum1 = added(sum1[:n_z], come1)
    with jax.named_scope("reduce_z"):
        part = jnp.concatenate(
            [sum0.reshape(n_z, 2, width), sum1.reshape(n_z, 1, width)], axis=1
        )
        part = lax.all_to_all(part, "z", split_axis=0, concat_axis=0, tiled=True)
        recon = jnp.sum(part.astype(f32), axis=0)
    low = (recon + jnp.concatenate([offset, offset1], axis=0)).astype(bf16)

    with jax.named_scope("gather_err"):
        low = gather_z(low)
        low0 = low[:, :2].reshape(-1, width)
        low1 = low[:, 2:].reshape(-1, width)
        rows0 = jnp.concatenate([low0, shift(low0, "y_lo", 1)], axis=0)
        rows1 = jnp.concatenate(gather_ring(low1, "x"), axis=0)
        errors1 = gather_ring(rows1, ring)
        errors0 = gather_ring(rows0, "x")
        other0 = [shift(e, "core", 1) for e in errors0]
        other1 = [shift(e, "core", 1) for e in errors1]

    own = source.astype(jnp.int32)[None]
    back, grad_dec, bias = grad_part(
        mine, mine_valid, own, acts, scale, decoders, errors0, errors1, None
    )
    grad_bdec = bias[0] + bias[1]
    others, grad_dec, _ = grad_part(
        theirs, theirs_valid, own, acts, scale, decoders, other0, other1, grad_dec
    )
    grad_enc, grad_benc = enc_part(turned, back, others, charge, positive, moved)
    return (grad_enc[None], grad_benc, grad_dec[None], grad_bdec)


def solution(mesh):
    parts = Mesh(
        mesh.devices.reshape(2, 2, 4, 8, 2), ("y_hi", "core", "x", "z", "y_lo")
    )
    layer = ("y_hi", "core")
    latent = ("x", "z", "y_lo")
    placed = (
        P(layer, latent, None),
        P(layer, latent, None),
        P(layer, None, latent),
        P(layer, latent),
        P(layer, None, latent, None),
        P(layer, None),
    )
    return jax.shard_map(
        local,
        mesh=parts,
        in_specs=placed,
        out_specs=(
            P(layer, None, latent),
            P(layer, latent),
            P(layer, None, latent, None),
            P(layer, None),
        ),
        check_vma=False,
    )
```

```python
import jax
import jax.numpy as jnp
from jax import lax
from jax.experimental import pallas as pl
from jax.experimental.pallas import tpu as pltpu
from jax.sharding import Mesh, PartitionSpec as P

penalty = 0.5
eps = 1e-06
bf16 = jnp.bfloat16
f32 = jnp.float32
grant = 16 << 20


def length(axis):
    names = axis if isinstance(axis, tuple) else (axis,)
    n = 1
    for name in names:
        n *= lax.axis_size(name)
    return n


def shift(v, axis, by):
    n = length(axis)
    return lax.ppermute(v, axis, [(i, (i + by) % n) for i in range(n)])


def gather_z(v):
    n = lax.axis_size("z")
    return lax.all_to_all(
        jnp.broadcast_to(v, (n, *v.shape)), "z", split_axis=0, concat_axis=0, tiled=True
    )


def gather_ring(v, axis):
    return [v] + [shift(v, axis, -d) for d in range(1, length(axis))]


def spec(shape, index):
    return pl.BlockSpec(shape, index)


def hold_kernel(when, w, out):
    pltpu.sync_copy(w, out)


def hold_part(when, w):
    return pl.pallas_call(
        hold_kernel,
        grid_spec=pltpu.PrefetchScalarGridSpec(
            num_scalar_prefetch=1,
            grid=(1,),
            in_specs=[pl.BlockSpec(memory_space=pl.ANY)],
            out_specs=pl.BlockSpec(memory_space=pltpu.VMEM),
        ),
        out_shape=jax.ShapeDtypeStruct(w.shape, w.dtype),
        cost_estimate=pl.CostEstimate(
            flops=w.size * 128, bytes_accessed=2 * w.size, transcendentals=0
        ),
        compiler_params=pltpu.CompilerParams(vmem_limit_bytes=grant),
        name="hold_part",
    )(when, w)


def product(valid, act, w):
    got = jnp.dot(act[...], w[0], preferred_element_type=f32)
    return jnp.where(valid[0] > 0, got, 0.0)


def give_kernel(order, valid, act, w, out):
    out[...] = product(valid, act, w).astype(bf16)


def keep_kernel(order, valid, act, w, got, *outs):
    total = (product(valid, act, w) + got[...].astype(f32)).astype(bf16)
    rows = outs[0].shape[0]
    for i, out in enumerate(outs):
        out[...] = total[i * rows : (i + 1) * rows]


def recon_part(target, valid, act, w, got=None, pieces=1):
    n, k = act.shape
    d = w.shape[2]
    wide = d
    rows = n // pieces
    ins = [
        spec((n, k), lambda j, o, v: (0, 0)),
        spec((1, k, wide), lambda j, o, v: (o[0], 0, j)),
    ]
    args = [target[None], valid[None], act, w]
    if got is not None:
        ins.append(spec((n, wide), lambda j, o, v: (0, j)))
        args.append(got)
    return pl.pallas_call(
        give_kernel if got is None else keep_kernel,
        grid_spec=pltpu.PrefetchScalarGridSpec(
            num_scalar_prefetch=2,
            grid=(1,),
            in_specs=ins,
            out_specs=[spec((rows, wide), lambda j, o, v: (0, j)) for _ in range(pieces)],
        ),
        out_shape=[jax.ShapeDtypeStruct((rows, d), bf16) for _ in range(pieces)],
        cost_estimate=pl.CostEstimate(
            flops=2 * n * k * d, bytes_accessed=2 * (n + k) * d, transcendentals=0
        ),
        compiler_params=pltpu.CompilerParams(vmem_limit_bytes=grant),
        name="recon_part",
    )(*args)


def side_kernel(valid, w, whole, act, turned, scale, charge, squares):
    j = pl.program_id(0)

    @pl.when(j == 0)
    def _():
        squares[...] = jnp.zeros_like(squares)

    for t in range(w.shape[0]):

        @pl.when(valid[t] > 0)
        def _():
            wide = w[t].astype(f32)
            squares[...] += jnp.sum(wide * wide, axis=1, keepdims=True)

    turned[...] = whole[...].T

    @pl.when(j == pl.num_programs(0) - 1)
    def _():
        norms = jnp.sqrt(squares[...] + eps)
        total = jnp.sum(act[...].astype(f32).T, axis=1, keepdims=True)
        scale[...] = penalty * total / norms
        charge[...] = (penalty * jnp.broadcast_to(norms, act.shape).T)[:1]


def side_part(valid, w, whole, act):
    n, k = act.shape
    t, _, d = w.shape
    wide = d // 4
    return pl.pallas_call(
        side_kernel,
        grid_spec=pltpu.PrefetchScalarGridSpec(
            num_scalar_prefetch=1,
            grid=(4,),
            in_specs=[
                spec((t, k, wide), lambda j, v: (0, 0, j)),
                spec((n, wide), lambda j, v: (0, j)),
                spec((n, k), lambda j, v: (0, 0)),
            ],
            out_specs=[
                spec((wide, n), lambda j, v: (j, 0)),
                spec((k, 1), lambda j, v: (0, 0)),
                spec((1, k), lambda j, v: (0, 0)),
            ],
            scratch_shapes=[pltpu.VMEM((k, 1), f32)],
        ),
        out_shape=[
            jax.ShapeDtypeStruct((d, n), bf16),
            jax.ShapeDtypeStruct((k, 1), f32),
            jax.ShapeDtypeStruct((1, k), f32),
        ],
        cost_estimate=pl.CostEstimate(
            flops=8 * n * k * d, bytes_accessed=2 * (t * k + 2 * n) * d, transcendentals=0
        ),
        compiler_params=pltpu.CompilerParams(vmem_limit_bytes=grant),
        name="side_part",
    )(valid, w, whole, act)


def grad_kernel(order, valid, own, act, scale, w, *refs):
    back, out, bias, whole = refs[-4:]
    i = pl.program_id(0)
    use = valid[i] > 0
    rows = refs[0].shape[0]

    for slot in range(2):

        @pl.when(use & (i == slot))
        def _():
            for p in range(4):
                whole[p * rows : (p + 1) * rows] = refs[slot * 4 + p][...]

    @pl.when(use)
    def _():
        e = whole[...]
        back[0] = lax.dot_general(
            e, w[0], (((1,), (1,)), ((), ())), preferred_element_type=f32
        )
        mse = lax.dot_general(
            act[0], e, (((0,), (0,)), ((), ())), preferred_element_type=f32
        )
        out[0] = (mse + scale[...] * w[0].astype(f32)).astype(bf16)

    @pl.when(own[0] == order[i])
    def _():
        bias[0] = jnp.sum(whole[...].astype(f32), axis=0, keepdims=True)

    @pl.when(jnp.logical_not(use))
    def _():
        back[...] = jnp.zeros_like(back)
        out[0] = jnp.zeros(out.shape[1:], bf16)

    @pl.when(own[0] != order[i])
    def _():
        bias[0] = jnp.zeros(bias.shape[1:], f32)


def grad_part(order, valid, own, act, scale, w, e0, e1, prior):
    slots, n, k = act.shape
    d = w.shape[2]
    extra = [] if prior is None else [prior]
    return pl.pallas_call(
        grad_kernel,
        grid_spec=pltpu.PrefetchScalarGridSpec(
            num_scalar_prefetch=3,
            grid=(slots,),
            in_specs=[
                spec((1, n, k), lambda i, o, v, s: (i, 0, 0)),
                spec((k, 1), lambda i, o, v, s: (0, 0)),
                spec((1, k, d), lambda i, o, v, s: (o[i], 0, 0)),
            ]
            + [spec((n // 4, d), lambda i, o, v, s: (0, 0)) for _ in range(8)]
            + [pl.BlockSpec(memory_space=pl.ANY) for _ in extra],
            out_specs=[
                spec((1, n, k), lambda i, o, v, s: (i, 0, 0)),
                spec((1, k, d), lambda i, o, v, s: (o[i], 0, 0)),
                spec((1, 1, d), lambda i, o, v, s: (i, 0, 0)),
            ],
            scratch_shapes=[pltpu.VMEM((n, d), bf16)],
        ),
        out_shape=[
            jax.ShapeDtypeStruct((slots, n, k), f32),
            jax.ShapeDtypeStruct(w.shape, bf16),
            jax.ShapeDtypeStruct((slots, 1, d), f32),
        ],
        input_output_aliases={} if prior is None else {14: 1},
        cost_estimate=pl.CostEstimate(
            flops=8 * n * k * d, bytes_accessed=12 * n * d, transcendentals=0
        ),
        compiler_params=pltpu.CompilerParams(vmem_limit_bytes=24 << 20),
        name="grad_part",
    )(order, valid, own, act, scale, w, *e0, *e1, *extra)


def enc_kernel(turned, mine, theirs, charge, positive, moved, out, bias, d_low):
    @pl.when(pl.program_id(0) == 0)
    def _():
        back = lax.dot_general(
            moved[...],
            mine[1] + theirs[1],
            (((0,), (0,)), ((), ())),
            precision=lax.Precision.HIGHEST,
            preferred_element_type=f32,
        )
        d_act = mine[0] + theirs[0] + back + charge[...]
        d_pre = d_act * 2.0 * positive[...]
        bias[...] = jnp.sum(d_pre, axis=0, keepdims=True)
        d_low[...] = d_pre.astype(bf16)

    out[...] = jnp.dot(turned[...], d_low[...], preferred_element_type=f32).astype(bf16)


def enc_part(turned, mine, theirs, charge, positive, moved):
    d, n = turned.shape
    k = charge.shape[1]
    steps = 4
    return pl.pallas_call(
        enc_kernel,
        grid=(steps,),
        in_specs=[
            spec((d // steps, n), lambda j: (j, 0)),
            spec((2, n, k), lambda j: (0, 0, 0)),
            spec((2, n, k), lambda j: (0, 0, 0)),
            spec((1, k), lambda j: (0, 0)),
            spec((n, k), lambda j: (0, 0)),
            spec((n, n), lambda j: (0, 0)),
        ],
        out_specs=[
            spec((d // steps, k), lambda j: (j, 0)),
            spec((1, k), lambda j: (0, 0)),
        ],
        out_shape=[
            jax.ShapeDtypeStruct((d, k), bf16),
            jax.ShapeDtypeStruct((1, k), f32),
        ],
        scratch_shapes=[pltpu.VMEM((n, k), bf16)],
        compiler_params=pltpu.CompilerParams(vmem_limit_bytes=grant),
        name="enc_part",
    )(turned, mine, theirs, charge, positive, moved)


def after(v, *earlier):
    return lax.optimization_barrier((v, *earlier))[0]


def added(first, rest):
    total = first.astype(f32)
    for v in rest:
        total = total + v.astype(f32)
    return total.astype(bf16)


def local(inputs, targets, w_enc, b_enc, w_dec, b_dec):
    high = lax.axis_index("y_hi")
    core = lax.axis_index("core")
    source = high * 2 + core
    decoders = w_dec[0]
    depth, k, width = decoders.shape
    n_x = lax.axis_size("x")
    n_z = lax.axis_size("z")
    mine = jnp.stack([core, core + 2]).astype(jnp.int32)
    theirs = jnp.stack([1 - core, 3 - core]).astype(jnp.int32)
    mine_valid = (mine >= source).astype(jnp.int32)
    theirs_valid = (theirs >= source).astype(jnp.int32)

    n = 2 * n_x * n_z * 2
    to = lax.broadcasted_iota(jnp.int32, (n, n), 0)
    at = lax.broadcasted_iota(jnp.int32, (n, n), 1)
    ahead = to // (n_x * n_z)
    row = (high * 2 + lax.axis_index("y_lo") + ahead) % 4 // 2
    place = to // n_z % n_x * (4 * n_z) + ahead % 2 * (2 * n_z) + to % n_z * 2 + row
    moved = lax.optimization_barrier((at == place).astype(f32))

    with jax.named_scope("gather_in"):
        rows = gather_z(inputs[0]).reshape(-1, width)
        rows = jnp.concatenate([rows, shift(rows, "y_lo", 1)], axis=0)
        decoders = hold_part(after(mine, rows), decoders)
        whole = jnp.concatenate(gather_ring(rows, "x"), axis=0)
    pre = jnp.dot(whole, w_enc[0], preferred_element_type=f32) + b_enc[0]
    positive = jnp.maximum(pre, 0.0)
    act = (positive * positive).astype(bf16)
    turned_act = jnp.dot(moved.astype(bf16), act, preferred_element_type=f32).astype(bf16)
    acts = jnp.stack([act, turned_act])

    (give1,) = recon_part(theirs[1], theirs_valid[1], turned_act, decoders)
    got1 = shift(give1, "core", 1)
    (give0,) = recon_part(theirs[0], theirs_valid[0], after(act, give1), decoders)
    got0 = shift(give0, "core", 1)
    part1 = recon_part(
        mine[1], mine_valid[1], after(turned_act, give0), decoders, got1, 4
    )
    part0 = recon_part(
        mine[0], mine_valid[0], after(act, part1[0]), decoders, got0, n_x
    )

    ring = ("y_hi", "y_lo")
    with jax.named_scope("reduce_one"):
        come0 = [shift(part0[d], "x", d) for d in range(1, n_x)]
        come1 = [shift(part1[d], ring, d) for d in range(1, 4)]
        all_valid = (jnp.arange(depth, dtype=jnp.int32) >= source).astype(jnp.int32)
        all_valid = after(all_valid, part0[0])
        turned, scale, charge = side_part(all_valid, decoders, whole, act)
        sum0 = added(part0[0], come0)
        sum1 = added(part1[0], come1)
        sum1 = after(sum1, scale)
    bias, aim = lax.optimization_barrier((b_dec, targets, sum0))[:2]
    offset = bias[0] - aim[0].astype(f32)
    with jax.named_scope("offset_hi"):
        offset1 = jnp.where(high == 0, shift(offset[:1], "y_hi", 1), offset[1:])
    with jax.named_scope("reduce_two"):
        half = sum0.shape[0] // 2
        come0 = shift(sum0[half:], "y_lo", 1)
        come1 = [shift(sum1[d * n_z : (d + 1) * n_z], "x", d) for d in range(1, n_x)]
        sum0 = added(sum0[:half], [come0])
        sum1 = added(sum1[:n_z], come1)
    with jax.named_scope("reduce_z"):
        part = jnp.concatenate(
            [sum0.reshape(n_z, 2, width), sum1.reshape(n_z, 1, width)], axis=1
        )
        part = lax.all_to_all(part, "z", split_axis=0, concat_axis=0, tiled=True)
        recon = jnp.sum(part.astype(f32), axis=0)
    low = (recon + jnp.concatenate([offset, offset1], axis=0)).astype(bf16)

    with jax.named_scope("gather_err"):
        low = gather_z(low)
        low0 = low[:, :2].reshape(-1, width)
        low1 = low[:, 2:].reshape(-1, width)
        rows0 = jnp.concatenate([low0, shift(low0, "y_lo", 1)], axis=0)
        rows1 = jnp.concatenate(gather_ring(low1, "x"), axis=0)
        errors1 = gather_ring(rows1, ring)
        errors0 = gather_ring(rows0, "x")
        other0 = [shift(e, "core", 1) for e in errors0]
        other1 = [shift(e, "core", 1) for e in errors1]

    own = source.astype(jnp.int32)[None]
    back, grad_dec, bias = grad_part(
        mine, mine_valid, own, acts, scale, decoders, errors0, errors1, None
    )
    grad_bdec = bias[0] + bias[1]
    others, grad_dec, _ = grad_part(
        theirs, theirs_valid, own, acts, scale, decoders, other0, other1, grad_dec
    )
    grad_enc, grad_benc = enc_part(turned, back, others, charge, positive, moved)
    return (grad_enc[None], grad_benc, grad_dec[None], grad_bdec)


def solution(mesh):
    parts = Mesh(
        mesh.devices.reshape(2, 2, 4, 8, 2), ("y_hi", "core", "x", "z", "y_lo")
    )
    layer = ("y_hi", "core")
    latent = ("x", "z", "y_lo")
    placed = (
        P(layer, latent, None),
        P(layer, latent, None),
        P(layer, None, latent),
        P(layer, latent),
        P(layer, None, latent, None),
        P(layer, None),
    )
    return jax.shard_map(
        local,
        mesh=parts,
        in_specs=placed,
        out_specs=(
            P(layer, None, latent),
            P(layer, latent),
            P(layer, None, latent, None),
            P(layer, None),
        ),
        check_vma=False,
    )
```
